32 devices in a mesh: rep: 4 (over z), px: 4 (over x, core), py: 2 (over y).
Axes of the slice: x: 2, y: 2, z: 4, core: 2. Of those that a mesh axis runs over, the one named last changes fastest.
Arguments:
- state: float32 [12, 2, 192, 96, 256], P('rep', None, 'px', 'py'), parts along dimension 0, may hold values from -6 to 6
- cotangent: float32 [12, 2, 192, 96, 256], P('rep', None, 'px', 'py'), parts along dimension 0, may hold values from -6 to 6
- w_in: bfloat16 [512, 192], replicated, may hold values from -0.4375 to 0.4375
- b_in: float32 [512], replicated, may hold values from -5 to 5
- w_out: bfloat16 [192, 512], replicated, may hold values from -0.25 to 0.25
Outputs:
- state_grad: float32 [12, 2, 192, 96, 256], P('rep', None, 'px', 'py'), parts along dimension 0
- grad_in: float32 [512, 768], P(('px', 'py'), 'rep'), parts along dimension 1
- grad_out: float32 [768, 512], P('rep', ('px', 'py')), parts along dimension 0
- grad_bias: float32 [4, 512], P('rep', ('px', 'py')), parts along dimension 0
The draws below stay inside these ranges and needn't reach their ends.
There are 4 independent parts, one for each index of `rep`. The reference program is written for one: setup_inputs(seed, part) draws one part's arguments, and reference() takes and returns one part's arrays. A program takes and returns all parts, laid end to end along the dimension named above; an argument that names none is the same for every part. Nothing has to cross between parts.
All inputs are finite; a program needn't handle non-finite values.
Results may differ from the reference program's by a relative error of at most 0.0065.
The reference program's roundings to bfloat16 on the way count: a program that leaves them out, or rounds other values in their place, can miss the bound.
Values may be sent and summed in bfloat16 or wider, within the bound.
A program may use at most 448 MiB of HBM per device.

```python
import math
import jax
import jax.numpy as jnp
from jax import lax

NG = 256
KY = 192
KZ = 96
PATCH = 4
FEAT = 192
HID = 512


def steps_of(rng, shape, cuts, smallest, largest):
    def one(position, blocks):
        heights = jax.random.uniform(jax.random.fold_in(jax.random.fold_in(rng, 6), position), (blocks,), jnp.float32, smallest / len(cuts), largest / len(cuts))
        return jnp.repeat(jnp.exp(heights), shape[position] // blocks).reshape((-1,) + (1,) * (len(shape) - position - 1))

    level = one(*cuts[0])
    for cut in cuts[1:]:
        level = level * one(*cut)
    return level


def centred(rng, dims, deviation, reach, pieces=(), held_as=jnp.bfloat16):
    drawn = jax.random.normal(rng, dims, jnp.float32) * deviation
    if len(pieces) > 0:
        drawn = steps_of(rng, dims, pieces, -0.22, 0.18) * drawn
    return jnp.clip(drawn, min=-reach, max=reach).astype(held_as)


def setup_inputs(seed: int = 0, part: int = 0) -> dict:
    seeds = jax.random.split(jax.random.key(seed), 6)
    own_keys = jax.random.split(jax.random.fold_in(seeds[5], part), 6)
    state = centred(own_keys[0], (3, 2, KY, KZ, NG), 1.3, 6.0, ((2, 4), (3, 2)), jnp.float32)
    cotangent = centred(own_keys[1], (3, 2, KY, KZ, NG), 1.0, 6.0, ((2, 4), (3, 2)), jnp.float32)
    w_in = centred(seeds[2], (HID, FEAT), FEAT ** -0.5, 0.4375)
    b_in = centred(seeds[3], (HID,), 1.0, 5.0, (), jnp.float32)
    w_out = centred(seeds[4], (FEAT, HID), HID ** -0.5, 0.25)
    return dict(state=state, cotangent=cotangent, w_in=w_in, b_in=b_in, w_out=w_out)


NU_DT = 5e-05
TIME_STEP = 0.01
FORCING = 20.0

def angles(leading, trailing, length):
    product = leading[:, None] * trailing[None, :] % length
    phases = product.astype(jnp.float32) * (2.0 * math.pi / length)
    factor = 1.0 / math.sqrt(length)
    return (jnp.cos(phases) * factor, jnp.sin(phases) * factor)

def mode_ids(count, length):
    counter = jnp.arange(count, dtype=jnp.int32)
    return jnp.where(counter < count // 2, counter, counter + length - count).astype(jnp.int32)

def mode_table(modes, length, direction):
    cosine, sine_part = angles(modes, jnp.arange(length, dtype=jnp.int32), length)
    top_rows = jnp.stack([cosine, direction * sine_part], axis=1)
    low_rows = jnp.stack([-direction * sine_part, cosine], axis=1)
    return jnp.stack([top_rows, low_rows], axis=0).astype(jnp.bfloat16)

def complex_table(length, direction):
    return mode_table(jnp.arange(length, dtype=jnp.int32), length, direction)

def real_table(length, mode_count):
    cosine, sine_part = angles(jnp.arange(mode_count, dtype=jnp.int32), jnp.arange(length, dtype=jnp.int32), length)
    return jnp.stack([cosine, -sine_part], axis=0).astype(jnp.bfloat16)

def rounded(values):
    return lax.optimization_barrier(values.astype(jnp.bfloat16)).astype(jnp.float32)

def signed(counter, length):
    return jnp.where(counter < length // 2, counter, counter - length).astype(jnp.float32)

def factors(ky_ids, kz_ids, length, ky_count):
    cutoff = length // 3
    wave_y = signed(ky_ids, ky_count)[:, None, None]
    wave_z = kz_ids.astype(jnp.float32)[None, :, None]
    wave_x = signed(jnp.arange(length, dtype=jnp.int32), length)[None, None, :]
    retained = ((jnp.abs(wave_x) <= cutoff) & (jnp.abs(wave_y) <= cutoff) & (wave_z <= cutoff)).astype(jnp.float32)
    square = wave_x * wave_x + wave_y * wave_y + wave_z * wave_z
    damping = jnp.exp(-NU_DT * square)
    weight = jnp.where(kz_ids[None, :, None] == 0, 1.0, 2.0).astype(jnp.float32)
    return ((wave_x, wave_y, wave_z), retained, damping, weight, square)

def cross(former, latter):
    return [former[1] * latter[2] - former[2] * latter[1], former[2] * latter[0] - former[0] * latter[2], former[0] * latter[1] - former[1] * latter[0]]

def curl_modes(waves, spectra):
    real_part = cross(waves, [spectra[slot, 0] for slot in range(3)])
    imag_part = cross(waves, [spectra[slot, 1] for slot in range(3)])
    return jnp.stack([jnp.stack([-imag_part[slot], real_part[slot]]) for slot in range(3)])

def project(waves, square, spectra):
    dotted = waves[0] * spectra[0] + waves[1] * spectra[1] + waves[2] * spectra[2]
    along_k = dotted / jnp.maximum(square, 1.0)
    return jnp.stack([spectra[slot] - waves[slot] * along_k for slot in range(3)])

def to_physical(spectra):
    length = spectra.shape[4]
    inverse = complex_table(length, 1.0).astype(jnp.float32)
    y_inverse = mode_table(mode_ids(spectra.shape[2], length), length, 1.0).astype(jnp.float32)
    z_table = real_table(length, spectra.shape[3]).astype(jnp.float32)
    sectioned = rounded(spectra)
    sectioned = rounded(jnp.einsum('cramn,rnsx->csamx', sectioned, inverse, precision=lax.Precision.HIGHEST))
    sectioned = rounded(jnp.einsum('csamx,saty->ctmxy', sectioned, y_inverse, precision=lax.Precision.HIGHEST))
    return jnp.einsum('ctmxy,tmz->cxyz', sectioned, z_table, precision=lax.Precision.HIGHEST).astype(jnp.bfloat16)

def to_spectral(field):
    length = field.shape[3]
    forward = complex_table(length, -1.0).astype(jnp.float32)
    y_forward = mode_table(mode_ids(KY, length), length, -1.0).astype(jnp.float32).transpose(0, 3, 2, 1)
    z_table = real_table(length, KZ).astype(jnp.float32)
    sectioned = field.astype(jnp.float32)
    sectioned = rounded(jnp.einsum('cxyz,rmz->crmxy', sectioned, z_table, precision=lax.Precision.HIGHEST))
    sectioned = rounded(jnp.einsum('crmxy,rysa->csamx', sectioned, y_forward, precision=lax.Precision.HIGHEST))
    return jnp.einsum('csamx,sxtn->ctamn', sectioned, forward, precision=lax.Precision.HIGHEST)

def to_boxes(field):
    channels, span_x, span_y, span_z = field.shape
    tiles = field.reshape(channels, span_x // PATCH, PATCH, span_y // PATCH, PATCH, span_z // PATCH, PATCH)
    return tiles.transpose(0, 2, 4, 6, 1, 3, 5).reshape(channels * PATCH ** 3, -1)

def from_boxes(box_values, layout):
    channels, span_x, span_y, span_z = layout
    tiles = box_values.reshape(channels, PATCH, PATCH, PATCH, span_x // PATCH, span_y // PATCH, span_z // PATCH)
    return tiles.transpose(0, 4, 1, 5, 2, 6, 3).reshape(layout)

def closure_terms(velocity, force_adj, w_in, b_in, w_out):
    features = to_boxes(velocity)
    adjoints = to_boxes(force_adj)
    pre_act = jnp.dot(w_in, features, preferred_element_type=jnp.float32) + b_in[:, None]
    hidden = jax.nn.silu(pre_act).astype(jnp.bfloat16)
    sigmoid = jax.nn.sigmoid(pre_act)
    hidden_adj = FORCING * jnp.dot(w_out.T, adjoints, preferred_element_type=jnp.float32)
    pre_adj = (hidden_adj * sigmoid * (1.0 + pre_act * (1.0 - sigmoid))).astype(jnp.bfloat16)
    grad_in = jnp.dot(pre_adj, features.T, preferred_element_type=jnp.float32)
    grad_out = FORCING * jnp.dot(adjoints, hidden.T, preferred_element_type=jnp.float32)
    grad_bias = lax.optimization_barrier(jnp.sum(pre_adj.astype(jnp.float32), axis=1))[None, :]
    feat_adj = jnp.dot(w_in.T, pre_adj, preferred_element_type=jnp.float32)
    return (from_boxes(feat_adj, velocity.shape), grad_in, grad_out, grad_bias)

def pointwise(feat_adj, velocity, vorticity, force_adj):
    vel_list = [velocity[slot].astype(jnp.float32) for slot in range(3)]
    vort_list = [vorticity[slot].astype(jnp.float32) for slot in range(3)]
    force_list = [force_adj[slot].astype(jnp.float32) for slot in range(3)]
    turned = cross(vort_list, force_list)
    vel_adj = jnp.stack([feat_adj[slot] + turned[slot] for slot in range(3)]).astype(jnp.bfloat16)
    vort_adj = jnp.stack(cross(force_list, vel_list)).astype(jnp.bfloat16)
    return (vel_adj, vort_adj)

def reference(state, cotangent, w_in, b_in, w_out):
    waves, retained, damping, weight, square = factors(jnp.arange(KY, dtype=jnp.int32), jnp.arange(KZ, dtype=jnp.int32), NG, KY)
    kept = retained * state
    spectra = weight * jnp.concatenate([kept, curl_modes(waves, kept)], axis=0)
    fields = to_physical(spectra)
    velocity, vorticity = (fields[:3], fields[3:])
    force_spec = TIME_STEP * retained * project(waves, square, damping * cotangent)
    force_adj = to_physical(force_spec)
    feat_adj, grad_in, grad_out, grad_bias = closure_terms(velocity, force_adj, w_in, b_in, w_out)
    vel_adj, vort_adj = pointwise(feat_adj, velocity, vorticity, force_adj)
    spectral = to_spectral(jnp.concatenate([vel_adj, vort_adj], axis=0))
    state_grad = damping * cotangent + weight * retained * (spectral[:3] + curl_modes(waves, spectral[3:]))
    return (state_grad, grad_in, grad_out, grad_bias)
```

```python
import functools
import itertools
import math

import jax
import jax.numpy as jnp
from jax import lax
from jax.experimental import pallas as pl
from jax.experimental.pallas import tpu as pltpu
from jax.sharding import PartitionSpec as P


PATCH = 4
VMEM_LIMIT = 66000000


NU_DT = 5e-05
TIME_STEP = 0.01
FORCING = 20.0


def angles(leading, trailing, length):
    product = leading[:, None] * trailing[None, :] % length
    phases = product.astype(jnp.float32) * (2.0 * math.pi / length)
    factor = 1.0 / math.sqrt(length)
    return (jnp.cos(phases) * factor, jnp.sin(phases) * factor)


def mode_ids(count, length):
    counter = jnp.arange(count, dtype=jnp.int32)
    return jnp.where(counter < count // 2, counter, counter + length - count)


def mode_table(modes, length, direction):
    cosine, sine_part = angles(modes, jnp.arange(length, dtype=jnp.int32), length)
    top_rows = jnp.stack([cosine, direction * sine_part], axis=1)
    low_rows = jnp.stack([-direction * sine_part, cosine], axis=1)
    return jnp.stack([top_rows, low_rows], axis=0).astype(jnp.bfloat16)


def complex_table(length, direction):
    return mode_table(jnp.arange(length, dtype=jnp.int32), length, direction)


def real_table(length, mode_count):
    cosine, sine_part = angles(
        jnp.arange(mode_count, dtype=jnp.int32), jnp.arange(length, dtype=jnp.int32), length
    )
    return jnp.stack([cosine, -sine_part], axis=0).astype(jnp.bfloat16)


def box_order(length, span):
    counter = jnp.arange(length, dtype=jnp.int32)
    local = counter % span
    rows = span // PATCH
    return counter - local + local % rows * PATCH + local // rows


def signed(counter, length):
    return jnp.where(counter < length // 2, counter, counter - length).astype(jnp.float32)


def factors(ky_ids, kz_ids, length, ky_count):
    cutoff = length // 3
    wave_y = signed(ky_ids, ky_count)[:, None, None]
    wave_z = kz_ids.astype(jnp.float32)[None, :, None]
    wave_x = signed(jnp.arange(length, dtype=jnp.int32), length)[None, None, :]
    retained = (
        (jnp.abs(wave_x) <= cutoff) & (jnp.abs(wave_y) <= cutoff) & (wave_z <= cutoff)
    ).astype(jnp.float32)
    square = wave_x * wave_x + wave_y * wave_y + wave_z * wave_z
    damping = jnp.exp(-NU_DT * square)
    weight = jnp.where(kz_ids[None, :, None] == 0, 1.0, 2.0).astype(jnp.float32)
    return ((wave_x, wave_y, wave_z), retained, damping, weight, square)


def cross(former, latter):
    return [
        former[1] * latter[2] - former[2] * latter[1],
        former[2] * latter[0] - former[0] * latter[2],
        former[0] * latter[1] - former[1] * latter[0],
    ]


def curl_modes(waves, spectra):
    real_part = cross(waves, [spectra[slot, 0] for slot in range(3)])
    imag_part = cross(waves, [spectra[slot, 1] for slot in range(3)])
    return jnp.stack([jnp.stack([-imag_part[slot], real_part[slot]]) for slot in range(3)])


def project(waves, square, spectra):
    dotted = waves[0] * spectra[0] + waves[1] * spectra[1] + waves[2] * spectra[2]
    along_k = dotted / jnp.maximum(square, 1.0)
    return jnp.stack([spectra[slot] - waves[slot] * along_k for slot in range(3)])


def to_physical(spectra):
    channels, paired, width_y, width_z, length = spectra.shape
    parts_x = lax.axis_size("px")
    parts_y = lax.axis_size("py")
    order_y = box_order(length, length)
    order_z = box_order(length, length)
    inverse = complex_table(length, 1.0)
    y_table = mode_table(mode_ids(width_y * parts_x, length), length, 1.0)[..., order_y].reshape(
        2, parts_x, width_y, 2, length
    )
    z_table = real_table(length, width_z * parts_y)[..., order_z].reshape(
        2, parts_y, width_z, length
    )
    flat = spectra.astype(jnp.bfloat16).reshape(channels, paired, width_y * width_z, length)
    along_x = jnp.einsum(
        "crpn,rnsx->csxp", flat, inverse, preferred_element_type=jnp.float32
    ).astype(jnp.bfloat16)
    along_x = along_x.reshape(channels, 2, length, 1, width_y * width_z)
    moved = lax.all_to_all(along_x, ("px", "py"), split_axis=2, concat_axis=3, tiled=True)
    blocks = moved.reshape(moved.shape[0], 2, moved.shape[2], parts_x, parts_y, width_y, width_z)
    along_y = jnp.einsum(
        "csxjlam,sjaty->cxtlmy", blocks, y_table, preferred_element_type=jnp.float32
    ).astype(jnp.bfloat16)
    return jnp.einsum(
        "cxtlmy,tlmz->cxyz", along_y, z_table, preferred_element_type=jnp.float32
    ).astype(jnp.bfloat16)


def to_spectral(field, ky_count, mode_count):
    channels, span_x, span_y, length = field.shape
    parts_x = lax.axis_size("px")
    parts_y = lax.axis_size("py")
    width_y = ky_count // parts_x
    width_z = mode_count // parts_y
    order_y = box_order(length, span_y)
    order_z = box_order(length, length)
    forward = complex_table(length, -1.0)
    y_table = (
        mode_table(mode_ids(ky_count, length), length, -1.0)
        .transpose(0, 3, 2, 1)[:, order_y]
        .reshape(2, length, 2, parts_x, width_y)
    )
    z_table = real_table(length, mode_count)[..., order_z].reshape(2, parts_y, width_z, length)
    along_z = jnp.einsum(
        "cxyz,rlmz->crlmxy", field, z_table, preferred_element_type=jnp.float32
    ).astype(jnp.bfloat16)
    along_y = jnp.einsum(
        "crlmxy,rysja->csxjlam", along_z, y_table, preferred_element_type=jnp.float32
    ).astype(jnp.bfloat16)
    along_y = along_y.reshape(channels, 2, span_x, parts_x * parts_y, width_y * width_z)
    moved = lax.all_to_all(along_y, ("px", "py"), split_axis=3, concat_axis=2, tiled=True)
    number = moved.shape[0]
    flat = moved.reshape(number, 2, length, -1)
    along_x = jnp.einsum("csxp,sxtn->ctpn", flat, forward, preferred_element_type=jnp.float32)
    return along_x.reshape(number, 2, width_y, width_z, length)


def to_boxes(field):
    channels, span_x, span_y, span_z = field.shape
    tiles = field.reshape(
        channels, span_x // PATCH, PATCH, PATCH, span_y // PATCH, PATCH, span_z // PATCH
    )
    return tiles.transpose(0, 2, 3, 5, 1, 4, 6).reshape(channels * PATCH**3, -1)


def from_boxes(box_values, layout):
    channels, span_x, span_y, span_z = layout
    tiles = box_values.reshape(
        channels, PATCH, PATCH, PATCH, span_x // PATCH, span_y // PATCH, span_z // PATCH
    )
    return tiles.transpose(0, 4, 1, 2, 5, 3, 6).reshape(layout)


def closure_terms(velocity, force_adj, w_in, b_in, w_out):
    features = to_boxes(velocity)
    adjoints = to_boxes(force_adj)
    pre_act = jnp.dot(w_in, features, preferred_element_type=jnp.float32) + b_in[:, None]
    hidden = jax.nn.silu(pre_act).astype(jnp.bfloat16)
    sigmoid = jax.nn.sigmoid(pre_act)
    hidden_adj = FORCING * jnp.dot(w_out.T, adjoints, preferred_element_type=jnp.float32)
    pre_adj = (hidden_adj * sigmoid * (1.0 + pre_act * (1.0 - sigmoid))).astype(jnp.bfloat16)
    grad_in = jnp.dot(pre_adj, features.T, preferred_element_type=jnp.float32)
    grad_out = FORCING * jnp.dot(adjoints, hidden.T, preferred_element_type=jnp.float32)
    grad_bias = jnp.sum(pre_adj.astype(jnp.float32), axis=1)[None, :]
    feat_adj = jnp.dot(w_in.T, pre_adj, preferred_element_type=jnp.float32).astype(jnp.bfloat16)
    feat_adj = lax.optimization_barrier(from_boxes(feat_adj, velocity.shape))
    return (feat_adj, grad_in, grad_out, grad_bias)


def field_cross(former, latter):
    return cross(
        [former[slot].astype(jnp.float32) for slot in range(3)],
        [latter[slot].astype(jnp.float32) for slot in range(3)],
    )


def shards(state, cotangent, w_in, b_in, w_out):
    width_y = state.shape[2]
    width_z = state.shape[3]
    length = state.shape[4]
    ky_count = width_y * lax.axis_size("px")
    ky_ids = lax.axis_index("px") * width_y + jnp.arange(width_y, dtype=jnp.int32)
    kz_ids = lax.axis_index("py") * width_z + jnp.arange(width_z, dtype=jnp.int32)
    waves, retained, damping, weight, square = factors(ky_ids, kz_ids, length, ky_count)
    kept = retained * state
    force_spec = TIME_STEP * retained * project(waves, square, damping * cotangent)
    modes = width_z * lax.axis_size("py")
    force_adj = to_physical(force_spec)
    velocity = to_physical(weight * kept)
    vorticity = to_physical(weight * curl_modes(waves, kept))
    vort_adj = jnp.stack(field_cross(force_adj, velocity)).astype(jnp.bfloat16)
    spec_vort = to_spectral(vort_adj, ky_count, modes)
    feat_adj, grad_in, grad_out, grad_bias = closure_terms(velocity, force_adj, w_in, b_in, w_out)
    turned = field_cross(vorticity, force_adj)
    vel_adj = jnp.stack([feat_adj[slot].astype(jnp.float32) + turned[slot] for slot in range(3)])
    spec_vel = to_spectral(vel_adj.astype(jnp.bfloat16), ky_count, modes)
    state_grad = damping * cotangent + weight * retained * (
        spec_vel + curl_modes(waves, spec_vort)
    )
    grad_in, grad_out, grad_bias = (
        lax.psum_scatter(grad_in, ("px", "py"), scatter_dimension=0, tiled=True),
        lax.psum_scatter(grad_out, ("px", "py"), scatter_dimension=1, tiled=True),
        lax.psum_scatter(grad_bias, ("px", "py"), scatter_dimension=1, tiled=True),
    )
    return (state_grad, grad_in, grad_out, grad_bias)


def dot(left, right):
    return lax.dot_general(
        left, right, (((1,), (0,)), ((), ())), preferred_element_type=jnp.float32
    )


def dot_t(left, right):
    return lax.dot_general(
        left, right, (((1,), (1,)), ((), ())), preferred_element_type=jnp.float32
    )


def spectral_kernel(
    ids_ref, state_ref, cot_ref, table_ref, *rest, dims, length, ky_count, chunk
):
    outs, (rows_ref, wide_ref) = rest[:-2], rest[-2:]
    width_y, block_z, dests = dims
    step = pl.program_id(0)
    cutoff = length // 3
    half = 2 * width_y
    halves = length // 128
    state = state_ref.reshape(6 * width_y * block_z * halves, 128)
    cot = cot_ref.reshape(6 * width_y * block_z * halves, 128)
    first_y = ids_ref[0]
    first_z = ids_ref[1]

    def put(field, row, side, re, im):
        re = re.astype(jnp.bfloat16)
        im = im.astype(jnp.bfloat16)
        base = field // 4 * (4 * half)
        tile = field % 4
        for slot, (left, right) in enumerate(((re, im), (im, -re))):
            place = slot * width_y + row
            if tile < 3:
                at = base + tile * 128 + place
            else:
                at = base + place // 32 * 128 + half + place % 32
            rows_ref[at : at + 16, side * 128 : side * 128 + 128] = left
            rows_ref[at : at + 16, length + side * 128 : length + side * 128 + 128] = right

    def plane(kz, carry):
        kz_id = first_z + step * block_z + kz
        start = kz // 8 * (8 * halves) + kz % 8
        wave_z = jnp.full((1, 1), kz_id, jnp.int32).astype(jnp.float32)
        keep_z = (wave_z <= cutoff).astype(jnp.float32)
        weight = jnp.where(wave_z == 0.0, 1.0, 2.0)
        for row, side in itertools.product(range(0, width_y, 16), range(halves)):
            lane = side * 128 + lax.broadcasted_iota(jnp.int32, (1, 128), 1)
            wave_x = jnp.where(lane < length // 2, lane, lane - length).astype(jnp.float32)
            keep_x = (jnp.abs(wave_x) <= cutoff).astype(jnp.float32)
            ky_id = first_y + row + lax.broadcasted_iota(jnp.int32, (16, 1), 0)
            wave_y = jnp.where(ky_id < ky_count // 2, ky_id, ky_id - ky_count).astype(jnp.float32)
            keep_y = (jnp.abs(wave_y) <= cutoff).astype(jnp.float32)
            kept = keep_y * keep_z * keep_x
            square = wave_x * wave_x + (wave_y * wave_y + wave_z * wave_z)
            damping = jnp.exp(-NU_DT * square)
            inverse = 1.0 / jnp.maximum(square, 1.0)
            scale = TIME_STEP * kept * damping

            def load(ref, c, part):
                at = ((c * 2 + part) * width_y + row) * block_z * halves + side * 8
                return ref[pl.ds(at + start, 16, stride=block_z * halves), :]

            force = []
            for part in range(2):
                v = [load(cot, c, part) for c in range(3)]
                along = (wave_x * v[0] + wave_y * v[1] + wave_z * v[2]) * inverse
                force.append(
                    [scale * (v[c] - k * along) for c, k in enumerate((wave_x, wave_y, wave_z))]
                )
            for c in range(3):
                put(c, row, side, force[0][c], force[1][c])
            factor = kept * weight
            for c in range(3):
                re = factor * load(state, c, 0)
                im = factor * load(state, c, 1)
                put(4 + c, row, side, re, im)
                if c > 0:
                    put(3 if c == 1 else 7, row, side, -wave_x * im, wave_x * re)
        lines = dot_t(table_ref[...], rows_ref[...])
        for tile in range(lines.shape[1] // 128):
            wide_ref[tile, pl.ds(kz, lines.shape[0], stride=block_z), :] = lines[
                :, tile * 128 : tile * 128 + 128
            ]
        return carry

    lax.fori_loop(0, block_z, plane, 0)
    slab = table_ref.shape[0] // dests
    for number, out in enumerate(outs):
        dest = ids_ref[2] ^ (number % dests)
        at = (dest * slab + number // dests * chunk) * block_z
        for x, tile in itertools.product(range(chunk), range(wide_ref.shape[0])):
            here = pl.ds(pl.multiple_of(at + x * block_z, block_z), block_z)
            out[x, :, tile * 128 : tile * 128 + 128] = wide_ref[tile, here, :].astype(
                jnp.bfloat16
            )


def tiled(field):
    c, parts, width_y, width_z, length = field.shape
    field = field.reshape(c, parts, width_y, width_z // 8, 8, length // 128, 128)
    return field.transpose(0, 1, 2, 3, 5, 4, 6)


def spectral_stage(ids, state, cotangent, table, dests, ky_count):
    _, _, width_y, width_z, length = state.shape
    state, cotangent = tiled(state), tiled(cotangent)
    chunk, block_z = 8, 16
    lanes = 16 * width_y
    block = pl.BlockSpec(
        (3, 2, width_y, block_z // 8, length // 128, 8, 128),
        lambda i, s: (0, 0, 0, i, 0, 0, 0),
    )
    return pl.pallas_call(
        functools.partial(
            spectral_kernel,
            dims=(width_y, block_z, dests),
            length=length,
            ky_count=ky_count,
            chunk=chunk,
        ),
        grid_spec=pltpu.PrefetchScalarGridSpec(
            num_scalar_prefetch=1,
            grid=(width_z // block_z,),
            in_specs=[block, block, pl.BlockSpec(table.shape, lambda i, s: (0, 0))],
            out_specs=[
                pl.BlockSpec((chunk, block_z, lanes), lambda i, s: (0, i, 0))
            ]
            * (length // chunk),
            scratch_shapes=[
                pltpu.VMEM((lanes, 2 * length), jnp.bfloat16),
                pltpu.VMEM((lanes // 128, length * block_z, 128), jnp.float32),
            ],
        ),
        out_shape=[jax.ShapeDtypeStruct((chunk, width_z, lanes), jnp.bfloat16)]
        * (length // chunk),
        compiler_params=pltpu.CompilerParams(vmem_limit_bytes=VMEM_LIMIT),
        cost_estimate=pl.CostEstimate(
            flops=2 * length * 2 * length * lanes * width_z,
            bytes_accessed=60000000,
            transcendentals=0,
        ),
        name="spectral_stage",
    )(ids, state, cotangent, table)


def physical_kernel(*refs, dims):
    parts_x, parts_y, width_y, width_z, length = dims
    devices = parts_x * parts_y
    datas = refs[:devices]
    out_refs = refs[devices + 14 : 2 * devices + 14]
    (
        y_ref,
        yk_ref,
        yt_ref,
        z_ref,
        zf_ref,
        yf_ref,
        kz_ref,
        ky_ref,
        w1_ref,
        w1t_ref,
        w2t_ref,
        b_ref,
        gi_ref,
        go_ref,
    ) = refs[devices : devices + 14]
    (
        gin_ref,
        gout_ref,
        force_ref,
        vel_ref,
        vort_ref,
        adj_ref,
        line_ref,
        point_ref,
        fore_ref,
        wide_ref,
        feat_ref,
        forc_ref,
        hid_ref,
        pre_ref,
    ) = refs[2 * devices + 14 :]
    group = 8 * width_y
    rows = 8 * width_z
    span = parts_y * width_z
    lane = lax.broadcasted_iota(jnp.int32, (1, 128), 1)
    low = lane < 64

    def source(py, lanes):
        return jnp.concatenate(
            [datas[px * parts_y + py][:, lanes] for px in range(parts_x)], axis=1
        )

    def tile_of(py, field):
        at = field // 4 * group + field % 4 * 128
        return source(py, slice(at, at + 128))

    def place(py, values):
        for dx in range(4):
            for ri in range(2):
                for pair in range(length // 128):
                    cols = slice(ri * length + pair * 128, ri * length + pair * 128 + 128)
                    near = values[dx * width_z : (dx + 1) * width_z, cols]
                    far = values[(4 + dx) * width_z : (5 + dx) * width_z, cols]
                    even = jnp.where(low, near, pltpu.roll(far, 64, 1))
                    odd = jnp.where(low, pltpu.roll(near, 64, 1), far)
                    at = dx * 2 * span + (py * 2 + ri) * width_z
                    cell = pair * 256
                    line_ref[at : at + width_z, cell : cell + 128] = even.astype(jnp.bfloat16)
                    line_ref[at : at + width_z, cell + 128 : cell + 256] = odd.astype(
                        jnp.bfloat16
                    )

    def finish(target, c):
        for dx in range(4):
            at = (c * 4 + dx) * length
            values = dot(z_ref[...], line_ref[dx * 2 * span : (dx + 1) * 2 * span, :])
            for dy in range(4):
                target[dy, at : at + length, :] = values[:, dy * 128 : dy * 128 + 128].astype(
                    target.dtype
                )

    for c in range(3):
        for py in range(parts_y):
            place(py, dot(tile_of(py, c), y_ref[...]))
        finish(force_ref, c)
    for c in range(3):
        for py in range(parts_y):
            values = dot(tile_of(py, 4 + c), y_ref[...])
            at = (c * parts_y + py) * rows
            for t in range(4):
                adj_ref[t, at : at + rows, :] = values[:, t * 128 : t * 128 + 128]
            place(py, values)
        finish(vel_ref, c)

    def held(c, py):
        at = (c * parts_y + py) * rows
        lines = [adj_ref[t, at : at + rows, :] for t in range(4)]
        return jnp.concatenate(lines[:2], axis=1), jnp.concatenate(lines[2:], axis=1)

    def slope_y(py, c):
        lines = tile_of(py, 4 + c)
        return dot(lines, yk_ref[0]) + dot(lines, yk_ref[1])

    for c in range(3):
        for py in range(parts_y):
            wave_z = kz_ref[py]
            if c == 0:
                re, im = held(1, py)
                values = slope_y(py, 2) - jnp.concatenate([-wave_z * im, wave_z * re], axis=1)
            elif c == 1:
                re, im = held(0, py)
                values = jnp.concatenate([-wave_z * im, wave_z * re], axis=1) - dot(
                    source(py, slice(group, 2 * group)), yt_ref[...]
                )
            else:
                values = dot(source(py, slice(0, group)), yt_ref[...]) - slope_y(py, 0)
            place(py, values)
        finish(vort_ref, c)

    gin_ref[...] = gi_ref[...]
    gout_ref[...] = go_ref[...]
    count = w1_ref.shape[1]
    hidden = w1_ref.shape[0]
    boxes = feat_ref.shape[1]
    several = boxes // 128
    cells = length // 4
    first = lax.broadcasted_iota(jnp.int32, (16, boxes), 0) == 0
    feat_ref[count : count + 16, :] = first.astype(jnp.bfloat16)

    def closure(step, carry):
        for k in range(several):
            bz = step * several + k
            for dy in range(4):
                at = pl.ds(bz, 48, stride=cells)
                feat_ref[dy * 48 : dy * 48 + 48, k * 128 : k * 128 + 128] = vel_ref[
                    dy, at, :
                ].astype(jnp.bfloat16)
                forc_ref[dy * 48 : dy * 48 + 48, k * 128 : k * 128 + 128] = force_ref[
                    dy, at, :
                ].astype(jnp.bfloat16)

        def units(part, inner):
            at = pl.ds(part * 128, 128)
            pre = dot(w1_ref[at, :], feat_ref[0:count, :]) + b_ref[at, :]
            sigma = 0.5 * jnp.tanh(0.5 * pre) + 0.5
            act = pre * sigma
            back = dot(w2t_ref[at, :], forc_ref[...])
            hid_ref[at, :] = act.astype(jnp.bfloat16)
            pre_ref[at, :] = (back * (FORCING * (sigma + act * (1.0 - sigma)))).astype(
                jnp.bfloat16
            )
            return inner

        lax.fori_loop(0, hidden // 128, units, 0)
        gin_ref[...] += dot_t(pre_ref[...], feat_ref[...])
        gout_ref[...] += dot_t(forc_ref[...], hid_ref[...])
        back = dot(w1t_ref[...], pre_ref[...])
        for k in range(several):
            bz = step * several + k
            for dy in range(4):
                adj_ref[dy, pl.ds(bz, 48, stride=cells), :] = back[
                    dy * 48 : dy * 48 + 48, k * 128 : k * 128 + 128
                ]
        return carry

    lax.fori_loop(0, cells // several, closure, 0)

    def crossing(dx, carry):
        def strip(part, inner):
            here = pl.ds(pl.multiple_of(part * 16, 16), 16)

            def at(c):
                return pl.ds(pl.multiple_of((c * 4 + dx) * length + part * 16, 16), 16)

            for dy in range(4):
                cols = slice(dy * 128, dy * 128 + 128)

                def rounded(ref):
                    return [
                        ref[dy, at(c), :].astype(jnp.bfloat16).astype(jnp.float32)
                        for c in range(3)
                    ]

                force = rounded(force_ref)
                for c, value in enumerate(cross(force, rounded(vel_ref))):
                    point_ref[3 + c, here, cols] = value.astype(jnp.bfloat16)
                for c, value in enumerate(cross(rounded(vort_ref), force)):
                    point_ref[c, here, cols] = (value + adj_ref[dy, at(c), :]).astype(
                        jnp.bfloat16
                    )
            return inner

        lax.fori_loop(0, length // 16, strip, 0)
        here = pl.ds(pl.multiple_of(dx * span, 16), span)
        for f in range(6):
            lines = dot(zf_ref[...], point_ref[f]).astype(jnp.bfloat16)
            fore_ref[f, here, 0 : 2 * length] = lines[0:span]
            fore_ref[f, here, 2 * length : 4 * length] = lines[span : 2 * span]
        return carry

    lax.fori_loop(0, 4, crossing, 0)

    sign = jnp.where(low, -1.0, 1.0)
    third = lane < width_y
    two_thirds = lane < 2 * width_y

    def backward(px):
        wave_y = ky_ref[px, 0:1, :]
        for pair in range(2):
            cols = slice(pair * 128, pair * 128 + 128)
            for dx in range(4):
                tops = slice(dx * span, (dx + 1) * span)
                u = [dot(fore_ref[f, tops, :], yf_ref[px, :, cols]) for f in range(6)]
                for py in range(parts_y):
                    part = slice(py * width_z, (py + 1) * width_z)
                    vel = [u[c][part] for c in range(3)]
                    vort = [u[3 + c][part] for c in range(3)]
                    wave_z = kz_ref[py, 0:width_z]
                    turned = sign * pltpu.roll(vort[0], 64, 1)
                    fields = [
                        vel[0]
                        + sign * pltpu.roll(wave_y * vort[2] - wave_z * vort[1], 64, 1),
                        vel[1] + wave_z * turned,
                        vel[2] - wave_y * turned,
                        vort[2],
                        vort[1],
                    ]
                    for ri in range(2):
                        back = 64 * ri

                        def moved(value, to):
                            shift = (to - back) % 128
                            return pltpu.roll(value, shift, 1) if shift else value

                        tail = jnp.where(
                            two_thirds,
                            jnp.where(
                                third, moved(fields[0], 0), moved(fields[1], width_y)
                            ),
                            moved(fields[4], 2 * width_y),
                        )
                        head = jnp.where(
                            two_thirds,
                            jnp.where(
                                third, moved(fields[2], 0), moved(fields[3], width_y)
                            ),
                            moved(fields[4], 2 * width_y - 32),
                        )
                        at = py * 16 * width_z + ri * 8 + pair * 4 + dx
                        wide_ref[0, pl.ds(at, width_z, stride=16), :] = tail
                        wide_ref[1, pl.ds(at, width_z, stride=16), :] = head
        for py in range(parts_y):
            for t in range(2):
                out_refs[px * parts_y + py][:, t * 128 : t * 128 + 128] = wide_ref[
                    t, py * 16 * width_z : (py + 1) * 16 * width_z, :
                ].astype(jnp.bfloat16)

    for px in range(parts_x):
        backward(px)


def physical_stage(data, tables, weights, sums, dims):
    parts_x, parts_y, _, width_z, length = dims
    hidden, count = weights[0].shape
    devices = parts_x * parts_y
    span = parts_y * width_z
    vmem = pl.BlockSpec(memory_space=pltpu.VMEM)
    operands = (*data, *tables, *weights, *sums)
    cells = 12 * length
    boxes = 512
    return pl.pallas_call(
        functools.partial(physical_kernel, dims=dims),
        in_specs=[vmem] * len(operands),
        out_specs=[vmem] * (devices + 2),
        out_shape=[
            *[jax.ShapeDtypeStruct((16 * width_z, 256), jnp.bfloat16)] * devices,
            jax.ShapeDtypeStruct(sums[0].shape, jnp.float32),
            jax.ShapeDtypeStruct(sums[1].shape, jnp.float32),
        ],
        scratch_shapes=[
            pltpu.VMEM((4, cells, 128), jnp.float32),
            pltpu.VMEM((4, cells, 128), jnp.float32),
            pltpu.VMEM((4, cells, 128), jnp.bfloat16),
            pltpu.VMEM((4, cells, 128), jnp.float32),
            pltpu.VMEM((4 * 2 * span, 512), jnp.bfloat16),
            pltpu.VMEM((6, length, 512), jnp.bfloat16),
            pltpu.VMEM((6, 4 * span, 4 * length), jnp.bfloat16),
            pltpu.VMEM((2, parts_y * 16 * width_z, 128), jnp.float32),
            pltpu.VMEM((count + 16, boxes), jnp.bfloat16),
            pltpu.VMEM((count, boxes), jnp.bfloat16),
            pltpu.VMEM((hidden, boxes), jnp.bfloat16),
            pltpu.VMEM((hidden, boxes), jnp.bfloat16),
        ],
        compiler_params=pltpu.CompilerParams(vmem_limit_bytes=VMEM_LIMIT),
        cost_estimate=pl.CostEstimate(
            flops=40000000000, bytes_accessed=20000000, transcendentals=0
        ),
        name="physical_stage",
    )(*operands)


def final_kernel(
    ids_ref, *rest, width_y, block_z, length, ky_count, chunks
):
    datas = rest[:chunks]
    cot_ref, eye_ref, table_ref, out_ref = rest[chunks:]
    step = pl.program_id(0)
    cutoff = length // 3
    halves = length // 128
    cot = cot_ref.reshape(6 * width_y * block_z * halves, 128)
    out = out_ref.reshape(6 * width_y * block_z * halves, 128)
    first_y = ids_ref[0]
    first_z = ids_ref[1]

    def plane(kz, carry):
        kz_id = first_z + step * block_z + kz
        wave_z = jnp.full((1, 1), kz_id, jnp.int32).astype(jnp.float32)
        keep_z = (wave_z <= cutoff).astype(jnp.float32)
        weight = jnp.where(wave_z == 0.0, 1.0, 2.0)
        here = pl.ds(pl.multiple_of(kz * 16, 16), 16)
        lines = jnp.concatenate(
            [data[here, :] for data in datas], axis=0
        )
        turned = dot_t(eye_ref[...], lines).astype(jnp.bfloat16)
        modes = dot(turned, table_ref[...])
        for row, side in itertools.product(range(0, width_y, 16), range(halves)):
            lane = side * 128 + lax.broadcasted_iota(jnp.int32, (1, 128), 1)
            wave_x = jnp.where(lane < length // 2, lane, lane - length).astype(jnp.float32)
            keep_x = (jnp.abs(wave_x) <= cutoff).astype(jnp.float32)
            ky_id = first_y + row + lax.broadcasted_iota(jnp.int32, (16, 1), 0)
            wave_y = jnp.where(ky_id < ky_count // 2, ky_id, ky_id - ky_count).astype(jnp.float32)
            keep_y = (jnp.abs(wave_y) <= cutoff).astype(jnp.float32)
            factor = keep_y * keep_z * keep_x * weight
            square = wave_x * wave_x + (wave_y * wave_y + wave_z * wave_z)
            damping = jnp.exp(-NU_DT * square)
            starts = [row, width_y + row, 128 + row, 128 + width_y + row]
            starts.append(2 * width_y + row if row < 32 else 128 + 2 * width_y + row - 32)
            cols = [part * length + side * 128 for part in range(2)]
            f = [[modes[at : at + 16, col : col + 128] for col in cols] for at in starts]
            spectra = [
                f[0],
                [f[1][0] + wave_x * f[3][1], f[1][1] - wave_x * f[3][0]],
                [f[2][0] - wave_x * f[4][1], f[2][1] + wave_x * f[4][0]],
            ]
            for c, part in itertools.product(range(3), range(2)):
                at = ((c * 2 + part) * width_y + row) * block_z * halves + side * 8
                where = pl.ds(at + kz, 16, stride=block_z * halves)
                out[where, :] = damping * cot[where, :] + factor * spectra[c][part]
        return carry

    lax.fori_loop(0, block_z, plane, 0)


def final_stage(ids, datas, cotangent, eye, table, ky_count):
    shape = cotangent.shape
    _, _, width_y, width_z, length = shape
    cotangent = tiled(cotangent)
    block_z = 8
    block = pl.BlockSpec(
        (3, 2, width_y, block_z // 8, length // 128, 8, 128),
        lambda i, s: (0, 0, 0, i, 0, 0, 0),
    )
    result = pl.pallas_call(
        functools.partial(
            final_kernel,
            width_y=width_y,
            block_z=block_z,
            length=length,
            ky_count=ky_count,
            chunks=len(datas),
        ),
        grid_spec=pltpu.PrefetchScalarGridSpec(
            num_scalar_prefetch=1,
            grid=(width_z // block_z,),
            in_specs=[
                pl.BlockSpec((16 * block_z, d.shape[1]), lambda i, s: (i, 0))
                for d in datas
            ]
            + [
                block,
                pl.BlockSpec(eye.shape, lambda i, s: (0, 0)),
                pl.BlockSpec(table.shape, lambda i, s: (0, 0)),
            ],
            out_specs=block,
        ),
        out_shape=jax.ShapeDtypeStruct(cotangent.shape, jnp.float32),
        compiler_params=pltpu.CompilerParams(vmem_limit_bytes=VMEM_LIMIT),
        cost_estimate=pl.CostEstimate(
            flops=2 * 256 * 512 * 512 * width_z, bytes_accessed=50000000, transcendentals=0
        ),
        name="final_stage",
    )(ids, *datas, cotangent, eye, table)
    return result.transpose(0, 1, 2, 3, 5, 4, 6).reshape(shape)


def order_of(length):
    counter = jnp.arange(length, dtype=jnp.int32)
    cells = length // PATCH
    return counter % cells * PATCH + counter // cells


def pairs(modes, places, length):
    cosine, sine_part = angles(modes, places, length)
    return cosine.astype(jnp.bfloat16), sine_part.astype(jnp.bfloat16)


def counted(me, parts, width):
    others = me ^ jnp.arange(parts, dtype=jnp.int32)
    return (others[:, None] * width + jnp.arange(width, dtype=jnp.int32)).reshape(-1)


def exchange(blocks, devices):
    moved = [blocks[0]]
    for k in range(1, devices):
        order = [(i, i ^ k) for i in range(devices)]
        moved.append(lax.ppermute(blocks[k], ("px", "py"), order))
    return moved


def fast_tables(dims, me_x, me_y):
    parts_x, parts_y, width_y, width_z, length = dims
    ky_count = parts_x * width_y
    grid = jnp.arange(length, dtype=jnp.int32)
    order = order_of(length)
    devices = parts_x * parts_y
    slab = length // devices

    cos_x, sin_x = pairs(grid, grid, length)
    enter = jnp.concatenate([cos_x, -sin_x], axis=1)

    ky = counted(me_x, parts_x, width_y)
    modes = jnp.where(ky < ky_count // 2, ky, ky + length - ky_count)
    wave_y = signed(ky, ky_count)
    cos_y, sin_y = pairs(modes, order, length)
    blocked = lambda t: t.reshape(parts_x, width_y, t.shape[-1])
    fill = 128 - 2 * width_y

    def lined(top, low):
        both = jnp.concatenate([blocked(top), blocked(low)], axis=1)
        return jnp.pad(both, ((0, 0), (0, fill), (0, 0))).reshape(parts_x * 128, -1)

    y_top = jnp.concatenate([cos_y, sin_y], axis=1)
    y_low = jnp.concatenate([-sin_y, cos_y], axis=1)
    y_table = lined(y_top, y_low)
    slope = wave_y[:, None]
    full = lined(slope * y_low.astype(jnp.float32), -slope * y_top.astype(jnp.float32))
    high = full.astype(jnp.bfloat16)
    rest = (full - high.astype(jnp.float32)).astype(jnp.bfloat16)
    y_slope = jnp.stack([high, rest])
    both = jnp.concatenate([blocked(y_top), blocked(y_low)], axis=1)
    both = both.reshape(parts_x, 3, 32, -1)
    y_split = jnp.pad(both, ((0, 0), (0, 0), (2 * width_y, 0), (0, 0))).reshape(
        parts_x * 384, -1
    )

    kz = counted(me_y, parts_y, width_z)
    cos_z, sin_z = pairs(order, kz, length)
    split = lambda t: t.reshape(length, parts_y, 1, width_z)
    z_table = jnp.concatenate([split(cos_z), split(-sin_z)], axis=2).reshape(length, -1)
    z_fore = jnp.concatenate([cos_z.T, -sin_z.T], axis=0)

    cos_f = blocked(cos_y).transpose(0, 2, 1)
    sin_f = blocked(sin_y).transpose(0, 2, 1)
    gap = jnp.zeros((parts_x, length, 64 - width_y), jnp.bfloat16)
    f_re = jnp.concatenate([cos_f, gap, -sin_f, gap], axis=2)
    f_im = jnp.concatenate([sin_f, gap, cos_f, gap], axis=2)

    def paired(t):
        t = t.reshape(parts_x, PATCH, 1, length // PATCH, 128)
        none = jnp.zeros_like(t)
        near = jnp.concatenate([t, none], axis=2).reshape(parts_x, 2 * length, 128)
        far = jnp.concatenate([none, t], axis=2).reshape(parts_x, 2 * length, 128)
        return jnp.concatenate([near, far], axis=2)

    y_fore = jnp.concatenate([paired(f_re), paired(f_im)], axis=1)

    wave_z = kz.astype(jnp.float32).reshape(parts_y, 1, width_z, 1)
    wave_z = jnp.broadcast_to(wave_z, (parts_y, 8, width_z, 1)).reshape(parts_y, -1, 1)
    line = jnp.pad(wave_y.reshape(parts_x, width_y), ((0, 0), (0, 64 - width_y)))
    wave_y = jnp.broadcast_to(
        jnp.concatenate([line, line], axis=1)[:, None, :], (parts_x, 8, 128)
    )

    chunks = slab // 8
    others = (me_x * parts_y + me_y) ^ jnp.arange(devices, dtype=jnp.int32)
    places = (
        others[None, :, None] * slab
        + jnp.arange(chunks, dtype=jnp.int32)[:, None, None] * 8
        + jnp.arange(8, dtype=jnp.int32)[None, None, :]
    ).reshape(-1)
    cos_l, sin_l = pairs(places, grid, length)
    top = jnp.concatenate([cos_l, -sin_l], axis=1).reshape(chunks * devices, 1, 8, -1)
    low = jnp.concatenate([sin_l, cos_l], axis=1).reshape(chunks * devices, 1, 8, -1)
    leave = jnp.concatenate([top, low], axis=1).reshape(2 * length, 2 * length)
    eye = jnp.eye(256, dtype=jnp.bfloat16)
    return (
        enter,
        (y_table, y_slope, y_split, z_table, z_fore, y_fore, wave_z, wave_y),
        leave,
        eye,
    )


def fast_shards(state, cotangent, w_in, b_in, w_out):
    parts_x = lax.axis_size("px")
    parts_y = lax.axis_size("py")
    _, _, width_y, width_z, length = state.shape
    hidden, count = w_in.shape
    devices = parts_x * parts_y
    dims = (parts_x, parts_y, width_y, width_z, length)
    ky_count = parts_x * width_y
    me_x, me_y = lax.axis_index("px"), lax.axis_index("py")
    ids = jnp.stack([me_x * width_y, me_y * width_z, me_x * parts_y + me_y]).astype(jnp.int32)
    enter, tables, leave, eye = fast_tables(dims, me_x, me_y)
    sent = spectral_stage(ids, state, cotangent, enter, devices, ky_count)
    boxed = (count // PATCH**3, PATCH, PATCH, PATCH)

    def by_row(w):
        return w.reshape(*boxed, hidden).transpose(2, 0, 1, 3, 4).reshape(count, hidden)

    w1t = by_row(w_in.T)
    w2 = by_row(w_out)
    weights = (w1t.T, w1t, w2.T, b_in[:, None])
    sums = (
        jnp.zeros((hidden, count + 16), jnp.float32),
        jnp.zeros((count, hidden), jnp.float32),
    )
    returned = []
    for j in range(0, len(sent), devices):
        moved = exchange(sent[j : j + devices], devices)
        moved = [block.reshape(8 * width_z, block.shape[-1]) for block in moved]
        *blocks, gin, gout = physical_stage(moved, tables, weights, sums, dims)
        sums = (gin, gout)
        returned += exchange(blocks, devices)
    state_grad = final_stage(ids, returned, cotangent, eye, leave, ky_count)
    total = jnp.concatenate([sums[0], FORCING * sums[1].T], axis=1)
    total = lax.psum_scatter(total, ("px", "py"), scatter_dimension=0, tiled=True)
    mixed = (PATCH, count // PATCH**3, PATCH, PATCH)

    def by_box(g):
        return g.reshape(-1, *mixed).transpose(0, 2, 3, 1, 4).reshape(-1, count)

    grad_in = by_box(total[:, :count])
    grad_bias = total[:, count][None, :]
    grad_out = by_box(total[:, count + 16 :]).T
    return (state_grad, grad_in, grad_out, grad_bias)


def choose(state, cotangent, w_in, b_in, w_out):
    _, _, width_y, width_z, length = state.shape
    devices = lax.axis_size("px") * lax.axis_size("py")
    fits = (
        state.shape[0] == 3
        and width_y == 48
        and lax.axis_size("px") == 4
        and lax.axis_size("py") == 2
        and width_z % 16 == 0
        and length == 256
        and length % (8 * devices) == 0
        and w_in.shape[1] == 3 * PATCH**3
        and w_in.shape[0] % 128 == 0
    )
    body = fast_shards if fits else shards
    return body(state, cotangent, w_in, b_in, w_out)


def solution(mesh):
    return jax.shard_map(
        choose,
        mesh=mesh,
        in_specs=(
            P("rep", None, "px", "py", None),
            P("rep", None, "px", "py", None),
            P(),
            P(),
            P(),
        ),
        out_specs=(
            P("rep", None, "px", "py", None),
            P(("px", "py"), "rep"),
            P("rep", ("px", "py")),
            P("rep", ("px", "py")),
        ),
        check_vma=False,
    )
```
